32 devices in a mesh: seg: 4 (over y, x), tile: 8 (over z, core).
Axes of the slice: x: 2, y: 2, z: 4, core: 2. Of those that a mesh axis runs over, the one named last changes fastest.
Arguments:
- starting_warmth: float32 [256, 65536], P('tile', 'seg'), may hold values from 0 to 1
- diffusivity_field: float32 [256, 65536], P('tile', 'seg'), may hold values from 0.1 to 1
- emitter_mask: int32 [256, 65536], P('tile', 'seg'), may hold values 0 or 1
Outputs:
- final_warmth: float32 [256, 65536], P('tile', 'seg')
The draws below stay inside these ranges and needn't reach their ends.
Inputs may be any that keep to these rules, and one draw needn't show every extreme that they name: `emitter_mask`: nonzero marks a source vertex.
All inputs are finite; a program needn't handle non-finite values. No bound on the sum of `emitter_mask` on one device may be relied on, other than what follows from the above.
Results may differ from the reference program's by a relative error of at most 0.00002.
Values sent between devices are 32-bit elements; how exact they have to be, the bound alone decides.
A program may use at most 128 MiB of HBM per device.

```python
import math
import jax
import jax.numpy as jnp

STEPS = 8
BAND_BREADTH = 256
BAND_EXTENT = 65536


def with_ends(values, rng, smallest, high):
    dims = values.shape
    index_at = [jax.random.randint(jax.random.fold_in(rng, axis), (), 0, dims[axis]) for axis in range(len(dims))]
    values = values.at[tuple(index_at)].set(smallest)
    longest = dims.index(max(dims))
    index_at[longest] = (index_at[longest] + 1) % dims[longest]
    return values.at[tuple(index_at)].set(high)


def block_scale(stream_key, shape, cuts, smallest, high):
    def one(axis_at, blocks):
        draws = jax.random.uniform(jax.random.fold_in(jax.random.fold_in(stream_key, 6), axis_at), (blocks,), jnp.float32, smallest / len(cuts), high / len(cuts))
        return jnp.repeat(jnp.exp(draws), shape[axis_at] // blocks).reshape((-1,) + (1,) * (len(shape) - axis_at - 1))

    loudness = one(*cuts[0])
    for cut in cuts[1:]:
        loudness = loudness * one(*cut)
    return loudness


def setup_inputs(seed: int = 0) -> dict:
    streams_of = jax.random.split(jax.random.key(seed), 4)
    return {
        "starting_warmth": jnp.clip(1.0 * jax.random.uniform(streams_of[0], (BAND_BREADTH, BAND_EXTENT), jnp.float32) ** block_scale(streams_of[0], (BAND_BREADTH, BAND_EXTENT), ((0, 8), (1, 4)), -0.2, 0.2), 0.0, 1.0),
        "diffusivity_field": jnp.clip(jnp.exp(math.log(1.0) - 2.3025851 * jax.random.uniform(streams_of[1], (BAND_BREADTH, BAND_EXTENT), jnp.float32) ** block_scale(streams_of[1], (BAND_BREADTH, BAND_EXTENT), ((0, 8), (1, 4)), -0.2, 0.2)), 0.1, 1.0),
        "emitter_mask": with_ends((jax.random.randint(streams_of[2], (BAND_BREADTH, BAND_EXTENT), 0, 64) < 1).astype(jnp.int32), jax.random.fold_in(streams_of[2], 1), 0, 1),
    }


time_step = 0.24


def advance(bordered_grid, conduct, source, interior_region):
    height = bordered_grid.shape[0] - 2
    length = bordered_grid.shape[1] - 2
    middle_point = bordered_grid[1:-1, 1:-1]
    self_conductance = conduct[1:-1, 1:-1]
    flux_sum = jnp.zeros_like(middle_point)
    for row_off, col_off in ((0, 1), (2, 1), (1, 0), (1, 2)):
        adjacent_cell = bordered_grid[row_off:row_off + height, col_off:col_off + length]
        near_conduct = conduct[row_off:row_off + height, col_off:col_off + length]
        flux_sum = flux_sum + 0.5 * (self_conductance + near_conduct) * (adjacent_cell - middle_point)
    updated = middle_point + time_step * flux_sum
    updated = jnp.where(source, jnp.float32(1.0), updated)
    if interior_region is not None:
        updated = updated * interior_region
    return updated


def reference(starting_warmth, diffusivity_field, emitter_mask):
    is_source = emitter_mask != 0
    conduct = jnp.pad(diffusivity_field, 1)
    present_warmth = starting_warmth
    for substep in range(STEPS):
        present_warmth = advance(jnp.pad(present_warmth, 1), conduct, is_source, None)
    return present_warmth
```

```python
import functools

import jax
import jax.numpy as jnp
from jax import lax
from jax.experimental import pallas as pl
from jax.experimental.pallas import tpu as pltpu
from jax.sharding import PartitionSpec as P

STEPS = 8
ROUNDS = (4, 4)
DEEP = max(ROUNDS)
STEP_SIZE = 0.24
LANES = 128
SUB = 8
MESH = pl.DeviceIdType.MESH


def kernel(
    sizes, u_hbm, k_hbm, s_hbm, out_hbm,
    u_nat, k_nat, s_nat, o_nat,
    u_0, u_a, u_b, k_row, s_row, c_e, c_w, c_n, c_s, c_0,
    col_out, col_in, corner_in, row_out, row_in,
    load_sem, store_sem, col_sems, corner_sems, first_sems, row_sems,
):
    rows, blocks, n_seg, n_tile = sizes
    groups = rows // SUB
    tiles = blocks // SUB
    seg, tile = lax.axis_index("seg"), lax.axis_index("tile")
    lane = lax.broadcasted_iota(jnp.int32, (SUB, LANES), 1)
    sublane = lax.broadcasted_iota(jnp.int32, (SUB, LANES), 0)
    first_lane, last_lane = lane == 0, lane == LANES - 1
    has_side = (seg > 0, seg < n_seg - 1)
    has_row = (tile > 0, tile < n_tile - 1)
    side_step = (-1, 1)
    left_at, right_at = SUB - 1, SUB + blocks
    halo_at = (left_at, right_at)
    edge_at = (SUB, SUB + blocks - 1)

    def both(a, b):
        return jnp.logical_and(a, b)

    barrier = pltpu.get_barrier_semaphore()
    count = jnp.int32(0)
    for ds in (-1, 0, 1):
        for dt in (-1, 0, 1):
            if ds == 0 and dt == 0:
                continue
            there = jnp.bool_(True)
            if ds:
                there = has_side[(ds + 1) // 2]
            if dt:
                there = both(there, has_row[(dt + 1) // 2])
            count = count + there.astype(jnp.int32)

            @pl.when(there)
            def _(ds=ds, dt=dt):
                pl.semaphore_signal(barrier, inc=1, device_id=(seg + ds, tile + dt), device_id_type=MESH)

    span = blocks * SUB
    sources = ((u_hbm, u_nat), (k_hbm, k_nat), (s_hbm, s_nat))
    order = [0, groups - 1] + list(range(1, groups - 1))

    def load(which, g):
        src, dst = sources[which]
        part = pl.ds(g * span, span)
        return pltpu.make_async_copy(src.at[part], dst.at[part], load_sem.at[which, g])

    for g in order:
        for which in range(3):
            load(which, g).start()

    zero_plane = jnp.zeros((SUB, LANES), jnp.float32)
    for side in range(2):
        top = 0 if side == 0 else DEEP + rows

        @pl.when(jnp.logical_not(has_row[side]))
        def _(top=top):
            def clear(j, c):
                at = pl.ds(j * SUB, SUB)
                for d in range(DEEP):
                    for ref in (u_0, k_row, s_row):
                        ref[top + d, at, :] = zero_plane
                return c

            lax.fori_loop(0, tiles + 2, clear, 0)

        @pl.when(jnp.logical_not(has_side[side]))
        def _(side=side):
            for r in range(rows + 2 * DEEP):
                for ref in (u_0, k_row, s_row):
                    ref[r, halo_at[side]:halo_at[side] + 1, :] = zero_plane[:1]

    def relayout(g):
        for which in range(3):
            load(which, g).wait()

        def body(j, c):
            for r in range(SUB):
                start = g * span + j * SUB * SUB + r
                at = pl.ds(SUB + j * SUB, SUB)
                row = DEEP + g * SUB + r
                u_0[row, at, :] = u_nat[pl.ds(start, SUB, stride=SUB), :]
                k_row[row, at, :] = k_nat[pl.ds(start, SUB, stride=SUB), :]
                s_row[row, at, :] = jnp.where(
                    s_nat[pl.ds(start, SUB, stride=SUB), :] != 0, jnp.float32(1.0), jnp.float32(0.0)
                )
            return c

        lax.fori_loop(0, tiles, body, 0)

    own = pl.ds(SUB, blocks)

    def first_copy(which, side):
        ref, deep = ((u_0, ROUNDS[0]), (k_row, DEEP), (s_row, DEEP))[which]
        if side == 0:
            src, dst = pl.ds(DEEP, deep), pl.ds(DEEP + rows, deep)
        else:
            src, dst = pl.ds(DEEP + rows - deep, deep), pl.ds(DEEP - deep, deep)
        return pltpu.make_async_remote_copy(
            src_ref=ref.at[src, own], dst_ref=ref.at[dst, own],
            send_sem=first_sems.at[0, which, side], recv_sem=first_sems.at[1, which, 1 - side],
            device_id=(seg, tile + side_step[side]), device_id_type=MESH,
        )

    def first_arrival(which, side):
        ref, deep = ((u_0, ROUNDS[0]), (k_row, DEEP), (s_row, DEEP))[which]
        dst = pl.ds(DEEP - deep, deep) if side == 0 else pl.ds(DEEP + rows, deep)
        return pltpu.make_async_remote_copy(
            src_ref=ref.at[dst, own], dst_ref=ref.at[dst, own],
            send_sem=first_sems.at[0, which, side], recv_sem=first_sems.at[1, which, side],
            device_id=(seg, tile + side_step[side]), device_id_type=MESH,
        )

    relayout(0)
    relayout(groups - 1)
    pl.semaphore_wait(barrier, count)
    for side in range(2):
        @pl.when(has_row[side])
        def _(side=side):
            for which in range(3):
                first_copy(which, side).start()

    def col_copy(side):
        return pltpu.make_async_remote_copy(
            src_ref=col_out.at[side], dst_ref=col_in.at[1 - side],
            send_sem=col_sems.at[0, side], recv_sem=col_sems.at[1, 1 - side],
            device_id=(seg + side_step[side], tile), device_id_type=MESH,
        )

    def corner_copy(side, vert):
        return pltpu.make_async_remote_copy(
            src_ref=col_out.at[side, 0 if vert == 0 else groups - 1],
            dst_ref=corner_in.at[1 - side, 1 - vert],
            send_sem=corner_sems.at[0, side, vert], recv_sem=corner_sems.at[1, 1 - side, 1 - vert],
            device_id=(seg + side_step[side], tile + side_step[vert]), device_id_type=MESH,
        )

    for g in range(1, groups - 1):
        relayout(g)
    row_refs = (u_0, k_row, s_row)
    for side in range(2):
        at = edge_at[side]
        for g in range(groups):
            for which, ref in enumerate(row_refs):
                for r in range(SUB):
                    col_out[side, g, which * SUB + r:which * SUB + r + 1, :] = ref[DEEP + g * SUB + r, at:at + 1, :]

        @pl.when(has_side[side])
        def _(side=side):
            col_copy(side).start()

        for vert in range(2):
            @pl.when(both(has_side[side], has_row[vert]))
            def _(side=side, vert=vert):
                corner_copy(side, vert).start()

    for side in range(2):
        @pl.when(has_side[side])
        def _(side=side):
            col_copy(1 - side).wait_recv()
            at = halo_at[side]
            for g in range(groups):
                for which, ref in enumerate(row_refs):
                    for r in range(SUB):
                        ref[DEEP + g * SUB + r, at:at + 1, :] = col_in[side, g, which * SUB + r:which * SUB + r + 1, :]

    def east(ref, row, base, here):
        beyond = ref[row, pl.ds(base + 1, SUB), :]
        return pltpu.roll(jnp.where(first_lane, beyond, here), LANES - 1, 1)

    def west(ref, row, base, here):
        beyond = ref[row, pl.ds(base - 1, SUB), :]
        return pltpu.roll(jnp.where(last_lane, beyond, here), 1, 1)

    half = jnp.float32(0.5 * STEP_SIZE)

    def prepare(lo, hi):
        def body(g, c):
            base = g * SUB + left_at
            at = pl.ds(base, SUB)
            column = seg * blocks + base - SUB + sublane
            inside_col = jnp.logical_and(column >= 0, column < n_seg * blocks)
            above, here = k_row[DEEP + lo - 1, at, :], k_row[DEEP + lo, at, :]
            for r in range(lo, hi):
                below = k_row[DEEP + r + 1, at, :]
                live = jnp.logical_and(inside_col, s_row[DEEP + r, at, :] == 0.0)
                if r < 0:
                    live = jnp.logical_and(live, has_row[0])
                if r >= rows:
                    live = jnp.logical_and(live, has_row[1])
                weight = jnp.where(live, half, jnp.float32(0.0))
                ce = weight * (here + east(k_row, DEEP + r, base, here))
                cw = weight * (here + west(k_row, DEEP + r, base, here))
                cn = weight * (here + above)
                cs = weight * (here + below)
                c_e[DEEP + r, at, :] = ce
                c_w[DEEP + r, at, :] = cw
                c_n[DEEP + r, at, :] = cn
                c_s[DEEP + r, at, :] = cs
                c_0[DEEP + r, at, :] = 1.0 - ((ce + cw) + (cn + cs))
                above, here = here, below
            return c

        lax.fori_loop(0, tiles + 1, body, 0)

    def advance(step, lo, hi):
        src, dst = (u_b, u_a) if step % 2 == 0 else (u_a, u_b)
        src = u_0 if step == 0 else src
        last = step == STEPS - 1

        def body(g, c):
            base = g * SUB + (SUB if last else left_at)
            at = pl.ds(base, SUB)
            above, here = src[DEEP + lo - 1, at, :], src[DEEP + lo, at, :]
            for r in range(lo, hi):
                below = src[DEEP + r + 1, at, :]
                row = DEEP + r
                new = (
                    (c_0[row, at, :] * here + c_n[row, at, :] * above)
                    + (c_s[row, at, :] * below + c_e[row, at, :] * east(src, row, base, here))
                    + c_w[row, at, :] * west(src, row, base, here)
                )
                if step == 0:
                    new = jnp.where(s_row[row, at, :] != 0.0, jnp.float32(1.0), new)
                if last:
                    start = (r // SUB) * span + g * SUB * SUB + r % SUB
                    o_nat[pl.ds(start, SUB, stride=SUB), :] = new
                else:
                    dst[row, at, :] = new
                above, here = here, below
            return c

        lax.fori_loop(0, tiles if last else tiles + 1, body, 0)

    def row_copy(which, side):
        d = ROUNDS[which]
        return pltpu.make_async_remote_copy(
            src_ref=row_out.at[which, side, pl.ds(0, d)], dst_ref=row_in.at[which, 1 - side, pl.ds(0, d)],
            send_sem=row_sems.at[0, which, side], recv_sem=row_sems.at[1, which, 1 - side],
            device_id=(seg, tile + side_step[side]), device_id_type=MESH,
        )

    def move_rows(src, src_row, dst, dst_row, d):
        def body(j, c):
            at = pl.ds(j * SUB, SUB)
            for i in range(d):
                dst[dst_row + i, at, :] = src[src_row + i, at, :]
            return c

        lax.fori_loop(0, tiles + 2, body, 0)

    def store(g):
        part = pl.ds(g * span, span)
        return pltpu.make_async_copy(o_nat.at[part], out_hbm.at[part], store_sem.at[g])

    done = 0
    prepare(1, rows - 1)
    for which, d in enumerate(ROUNDS):
        if which:
            cur = u_a if done % 2 == 1 else u_b
            for side in range(2):
                move_rows(cur, DEEP if side == 0 else DEEP + rows - d, row_out.at[which, side], 0, d)

                @pl.when(has_row[side])
                def _(which=which, side=side):
                    row_copy(which, side).start()

        for j in range(1, d + 1):
            advance(done + j - 1, j, rows - j)
        if which == len(ROUNDS) - 1:
            for g in range(1, groups - 1):
                if g * SUB >= d and (g + 1) * SUB <= rows - d:
                    store(g).start()

        if which == 0:
            for side in range(2):
                @pl.when(has_row[side])
                def _(side=side):
                    for w in range(3):
                        first_arrival(w, side).wait_recv()
                        first_copy(w, side).wait_send()

            for side in range(2):
                for vert in range(2):
                    corner = both(has_side[side], has_row[vert])
                    at = halo_at[side]

                    @pl.when(corner)
                    def _(side=side, vert=vert, at=at):
                        corner_copy(1 - side, 1 - vert).wait_recv()
                        for w, ref in enumerate(row_refs):
                            for i in range(DEEP):
                                from_row = w * SUB + (SUB - DEEP + i if vert == 0 else i)
                                to_row = i if vert == 0 else DEEP + rows + i
                                ref[to_row, at:at + 1, :] = corner_in[side, vert, from_row:from_row + 1, :]
            prepare(1 - DEEP, 1)
            prepare(rows - 1, rows + DEEP - 1)
        else:
            for side in range(2):
                top = DEEP - d if side == 0 else DEEP + rows

                @pl.when(has_row[side])
                def _(which=which, side=side, top=top, cur=cur, d=d):
                    row_copy(which, 1 - side).wait_recv()
                    move_rows(row_in.at[which, side], 0, cur, top, d)

                @pl.when(jnp.logical_not(has_row[side]))
                def _(top=top, cur=cur, d=d):
                    def clear(j, c):
                        for i in range(d):
                            cur[top + i, pl.ds(j * SUB, SUB), :] = zero_plane
                        return c

                    lax.fori_loop(0, tiles + 2, clear, 0)

        for j in range(1, d + 1):
            final = done + j == STEPS
            advance(done + j - 1, 0 if final else j - d, j)
            advance(done + j - 1, rows - j, rows if final else rows - j + d)
        done += d

    for g in range(groups):
        if not (g * SUB >= d and (g + 1) * SUB <= rows - d):
            store(g).start()
    for side in range(2):
        @pl.when(has_side[side])
        def _(side=side):
            col_copy(side).wait_send()

        for vert in range(2):
            @pl.when(both(has_side[side], has_row[vert]))
            def _(side=side, vert=vert):
                corner_copy(side, vert).wait_send()

        @pl.when(has_row[side])
        def _(side=side):
            for which in range(1, len(ROUNDS)):
                row_copy(which, side).wait_send()
    for g in range(groups):
        store(g).wait()


def shards(n_seg, n_tile, warmth, conductivity, sources):
    rows, columns = warmth.shape
    blocks = columns // LANES
    groups = rows // SUB

    def planes(a):
        return a.reshape(groups, SUB, blocks, LANES).transpose(0, 2, 1, 3).reshape(-1, LANES)

    flat = rows * blocks
    f32 = jnp.float32
    plane = (rows + 2 * DEEP, blocks + 2 * SUB, LANES)
    vmem = pltpu.VMEM
    sem = pltpu.SemaphoreType.DMA
    n = len(ROUNDS)
    out = pl.pallas_call(
        functools.partial(kernel, (rows, blocks, n_seg, n_tile)),
        out_shape=jax.ShapeDtypeStruct((flat, LANES), f32),
        in_specs=[pl.BlockSpec(memory_space=pl.ANY)] * 3,
        out_specs=pl.BlockSpec(memory_space=pl.ANY),
        scratch_shapes=[
            vmem((flat, LANES), f32), vmem((flat, LANES), f32), vmem((flat, LANES), sources.dtype), vmem((flat, LANES), f32),
        ] + [vmem(plane, f32)] * 10 + [
            vmem((2, groups, 3 * SUB, LANES), f32), vmem((2, groups, 3 * SUB, LANES), f32),
            vmem((2, 2, 3 * SUB, LANES), f32),
            vmem((n, 2, DEEP, blocks + 2 * SUB, LANES), f32), vmem((n, 2, DEEP, blocks + 2 * SUB, LANES), f32),
            sem((3, groups)), sem((groups,)), sem((2, 2)), sem((2, 2, 2)), sem((2, 3, 2)), sem((2, n, 2)),
        ],
        compiler_params=pltpu.CompilerParams(
            collective_id=0, has_side_effects=True, vmem_limit_bytes=60 * 1024 * 1024
        ),
    )(planes(warmth), planes(conductivity), planes(sources))
    return out.reshape(groups, blocks, SUB, LANES).transpose(0, 2, 1, 3).reshape(rows, columns)


def solution(mesh):
    spec = P("tile", "seg")
    return jax.shard_map(
        functools.partial(shards, mesh.shape["seg"], mesh.shape["tile"]),
        mesh=mesh,
        in_specs=(spec, spec, spec),
        out_specs=spec,
        check_vma=False,
    )
```

```python
import functools

import jax
import jax.numpy as jnp
from jax import lax
from jax.experimental import pallas as pl
from jax.experimental.pallas import tpu as pltpu
from jax.sharding import PartitionSpec as P

STEPS = 8
ROUNDS = (4, 4)
DEEP = max(ROUNDS)
STEP_SIZE = 0.24
LANES = 128
SUB = 8
MESH = pl.DeviceIdType.MESH

PAD = 8
TERMS = 5


def kernel(
    sizes, u_hbm, k_hbm, s_hbm, out_hbm,
    u_nat, k_nat, s_nat, o_nat,
    u_0, u_a, u_b, k_row, s_row, coef,
    col_out, col_in, corner_in, row_out, row_in,
    load_sem, store_sem, col_sems, corner_sems, first_sems, row_sems,
):
    rows, blocks, n_seg, n_tile = sizes
    groups = rows // SUB
    tiles = blocks // SUB
    seg, tile = lax.axis_index("seg"), lax.axis_index("tile")
    lane = lax.broadcasted_iota(jnp.int32, (SUB, LANES), 1)
    sublane = lax.broadcasted_iota(jnp.int32, (SUB, LANES), 0)
    first_lane, last_lane = lane == 0, lane == LANES - 1
    has_side = (seg > 0, seg < n_seg - 1)
    has_row = (tile > 0, tile < n_tile - 1)
    side_step = (-1, 1)
    own_at = PAD + SUB
    halo_at = (PAD, own_at + LANES)
    edge_at = (own_at, own_at + LANES - SUB)
    edge_lane = (first_lane, last_lane)
    edge_id = (0, LANES - 1)
    parts = LANES // SUB
    length = LANES + 2 * SUB + 2 * PAD
    zero = jnp.float32(0.0)

    def both(a, b):
        return jnp.logical_and(a, b)

    barrier = pltpu.get_barrier_semaphore()
    count = jnp.int32(0)
    for ds in (-1, 0, 1):
        for dt in (-1, 0, 1):
            if ds == 0 and dt == 0:
                continue
            there = jnp.bool_(True)
            if ds:
                there = has_side[(ds + 1) // 2]
            if dt:
                there = both(there, has_row[(dt + 1) // 2])
            count = count + there.astype(jnp.int32)

            @pl.when(there)
            def _(ds=ds, dt=dt):
                pl.semaphore_signal(barrier, inc=1, device_id=(seg + ds, tile + dt), device_id_type=MESH)

    span = blocks * SUB
    sources = ((u_hbm, u_nat), (k_hbm, k_nat), (s_hbm, s_nat))
    order = [0, groups - 1] + list(range(1, groups - 1))

    def load(which, g):
        src, dst = sources[which]
        part = pl.ds(g * span, span)
        return pltpu.make_async_copy(src.at[part], dst.at[part], load_sem.at[which, g])

    for g in order:
        for which in range(3):
            load(which, g).start()

    zero_plane = jnp.zeros((SUB, LANES), jnp.float32)
    for side in range(2):
        top = 0 if side == 0 else DEEP + rows

        @pl.when(jnp.logical_not(has_row[side]))
        def _(top=top):
            def clear(j, c):
                at = pl.ds(j * SUB, SUB)
                for d in range(DEEP):
                    for ref in (u_0, k_row, s_row):
                        ref[top + d, at, :] = zero_plane
                return c

            lax.fori_loop(0, length // SUB, clear, 0)

    row_refs = (u_0, k_row, s_row)
    own = pl.ds(own_at, LANES)

    def neighbour_run(end, side):
        return jnp.where(edge_lane[side], zero, pltpu.roll(end, (1, LANES - 1)[side], 1))

    def relayout(g):
        for which in range(3):
            load(which, g).wait()

        def body(r, c):
            at = pl.ds(g * span + r, LANES, stride=SUB)
            row = DEEP + g * SUB + r
            for which, ref in enumerate(row_refs):
                plane = (u_nat, k_nat, s_nat)[which][at, :]
                if which == 2:
                    plane = jnp.where(plane != 0, jnp.float32(1.0), zero)
                plane = plane.T
                ref[row, own, :] = plane
                ref[row, halo_at[0]:halo_at[0] + SUB, :] = neighbour_run(plane[-SUB:], 0)
                ref[row, halo_at[1]:halo_at[1] + SUB, :] = neighbour_run(plane[:SUB], 1)
            return c

        lax.fori_loop(0, SUB, body, 0, unroll=2)


    def first_copy(which, side):
        ref, deep = ((u_0, ROUNDS[0]), (k_row, DEEP), (s_row, DEEP))[which]
        if side == 0:
            src, dst = pl.ds(DEEP, deep), pl.ds(DEEP + rows, deep)
        else:
            src, dst = pl.ds(DEEP + rows - deep, deep), pl.ds(DEEP - deep, deep)
        return pltpu.make_async_remote_copy(
            src_ref=ref.at[src, own], dst_ref=ref.at[dst, own],
            send_sem=first_sems.at[0, which, side], recv_sem=first_sems.at[1, which, 1 - side],
            device_id=(seg, tile + side_step[side]), device_id_type=MESH,
        )

    def first_arrival(which, side):
        ref, deep = ((u_0, ROUNDS[0]), (k_row, DEEP), (s_row, DEEP))[which]
        dst = pl.ds(DEEP - deep, deep) if side == 0 else pl.ds(DEEP + rows, deep)
        return pltpu.make_async_remote_copy(
            src_ref=ref.at[dst, own], dst_ref=ref.at[dst, own],
            send_sem=first_sems.at[0, which, side], recv_sem=first_sems.at[1, which, side],
            device_id=(seg, tile + side_step[side]), device_id_type=MESH,
        )

    relayout(0)
    relayout(groups - 1)
    pl.semaphore_wait(barrier, count)
    for side in range(2):
        @pl.when(has_row[side])
        def _(side=side):
            for which in range(3):
                first_copy(which, side).start()

    def col_copy(side):
        return pltpu.make_async_remote_copy(
            src_ref=col_out.at[side], dst_ref=col_in.at[1 - side],
            send_sem=col_sems.at[0, side], recv_sem=col_sems.at[1, 1 - side],
            device_id=(seg + side_step[side], tile), device_id_type=MESH,
        )

    def corner_copy(side, vert):
        return pltpu.make_async_remote_copy(
            src_ref=col_out.at[side],
            dst_ref=corner_in.at[1 - side, 1 - vert],
            send_sem=corner_sems.at[0, side, vert], recv_sem=corner_sems.at[1, 1 - side, 1 - vert],
            device_id=(seg + side_step[side], tile + side_step[vert]), device_id_type=MESH,
        )

    for g in range(1, groups - 1):
        relayout(g)
    for side in range(2):
        for which, ref in enumerate(row_refs):
            packed = jnp.zeros((SUB, LANES), jnp.float32)
            for r in range(rows):
                end = ref[DEEP + r, edge_at[side]:edge_at[side] + SUB, :]
                packed = jnp.where(lane == r, pltpu.roll(end, (r - edge_id[side]) % LANES, 1), packed)
            col_out[side, which * SUB:(which + 1) * SUB, :] = packed

        @pl.when(has_side[side])
        def _(side=side):
            col_copy(side).start()

        for vert in range(2):
            @pl.when(both(has_side[side], has_row[vert]))
            def _(side=side, vert=vert):
                corner_copy(side, vert).start()

    def unpack(ref, side, packed, pairs):
        at = slice(halo_at[side], halo_at[side] + SUB)
        for r, row in pairs:
            end = pltpu.roll(packed, (edge_id[side] - r) % LANES, 1)
            ref[row, at, :] = jnp.where(edge_lane[side], end, ref[row, at, :])

    for side in range(2):
        @pl.when(has_side[side])
        def _(side=side):
            col_copy(1 - side).wait_recv()
            for which, ref in enumerate(row_refs):
                unpack(ref, side, col_in[side, which * SUB:(which + 1) * SUB, :], [(r, DEEP + r) for r in range(rows)])

    half = jnp.float32(0.5 * STEP_SIZE)

    def prepare(lo, hi):
        def body(g, c):
            base = pl.multiple_of(g * SUB, SUB) + PAD
            at = pl.ds(base, SUB)
            cell = base - own_at + sublane
            outside = both(both(seg == 0, first_lane), cell < 0)
            outside = jnp.logical_or(outside, both(both(seg == n_seg - 1, last_lane), cell >= LANES))
            above, here = k_row[DEEP + lo - 1, at, :], k_row[DEEP + lo, at, :]
            for r in range(lo, hi):
                row = DEEP + r
                below = k_row[row + 1, at, :]
                live = both(jnp.logical_not(outside), s_row[row, at, :] == 0.0)
                if r < 0:
                    live = both(live, has_row[0])
                if r >= rows:
                    live = both(live, has_row[1])
                weight = jnp.where(live, half, zero)
                cw = weight * (here + k_row[row, pl.ds(base - 1, SUB), :])
                ce = weight * (here + k_row[row, pl.ds(base + 1, SUB), :])
                cn = weight * (here + above)
                cs = weight * (here + below)
                for i, term in enumerate((ce, cw, cn, cs, 1.0 - ((ce + cw) + (cn + cs)))):
                    coef[row, pl.ds(pl.multiple_of(g * (TERMS * SUB), SUB) + i * SUB, SUB), :] = term
                above, here = here, below
            return c

        lax.fori_loop(0, parts + 2, body, 0)

    def advance(step, *ranges):
        src, dst = (u_b, u_a) if step % 2 == 0 else (u_a, u_b)
        src = u_0 if step == 0 else src
        last = step == STEPS - 1

        def body(g, c):
            base = pl.multiple_of(g * SUB, SUB) + PAD
            at = pl.ds(base, SUB)
            for lo, hi in ranges:
                above, here = src[DEEP + lo - 1, at, :], src[DEEP + lo, at, :]
                for r in range(lo, hi):
                    row = DEEP + r
                    below = src[row + 1, at, :]
                    ce, cw, cn, cs, c0 = (
                        coef[row, pl.ds(pl.multiple_of(g * (TERMS * SUB), SUB) + i * SUB, SUB), :] for i in range(TERMS)
                    )
                    new = (
                        (c0 * here + cn * above)
                        + (cs * below + ce * src[row, pl.ds(base + 1, SUB), :])
                        + cw * src[row, pl.ds(base - 1, SUB), :]
                    )
                    if step == 0:
                        new = jnp.where(s_row[row, at, :] != 0.0, jnp.float32(1.0), new)
                    dst[row, at, :] = new
                    above, here = here, below
            return c

        lax.fori_loop(1 if last else 0, parts + (1 if last else 2), body, 0)

    def give_back(g):
        done_ref = u_b if STEPS % 2 == 0 else u_a

        def body(r, c):
            o_nat[pl.ds(g * span + r, LANES, stride=SUB), :] = done_ref[DEEP + g * SUB + r, own, :].T
            return c

        lax.fori_loop(0, SUB, body, 0, unroll=2)
        store(g).start()

    def row_copy(which, side):
        d = ROUNDS[which]
        return pltpu.make_async_remote_copy(
            src_ref=row_out.at[which, side, pl.ds(0, d)], dst_ref=row_in.at[which, 1 - side, pl.ds(0, d)],
            send_sem=row_sems.at[0, which, side], recv_sem=row_sems.at[1, which, 1 - side],
            device_id=(seg, tile + side_step[side]), device_id_type=MESH,
        )

    def move_rows(src, src_row, dst, dst_row, d):
        def body(j, c):
            at = pl.ds(j * SUB, SUB)
            for i in range(d):
                dst[dst_row + i, at, :] = src[src_row + i, at, :]
            return c

        lax.fori_loop(0, length // SUB, body, 0)

    def store(g):
        part = pl.ds(g * span, span)
        return pltpu.make_async_copy(o_nat.at[part], out_hbm.at[part], store_sem.at[g])

    done = 0
    prepare(1, rows - 1)
    for which, d in enumerate(ROUNDS):
        if which:
            cur = u_a if done % 2 == 1 else u_b
            for side in range(2):
                move_rows(cur, DEEP if side == 0 else DEEP + rows - d, row_out.at[which, side], 0, d)

                @pl.when(has_row[side])
                def _(which=which, side=side):
                    row_copy(which, side).start()

        for j in range(1, d + 1):
            advance(done + j - 1, (j, rows - j))
        if which == len(ROUNDS) - 1:
            for g in range(1, groups - 1):
                if g * SUB >= d and (g + 1) * SUB <= rows - d:
                    give_back(g)

        if which == 0:
            for side in range(2):
                @pl.when(has_row[side])
                def _(side=side):
                    for w in range(3):
                        first_arrival(w, side).wait_recv()
                        first_copy(w, side).wait_send()

            for vert in range(2):
                top = 0 if vert == 0 else DEEP + rows

                @pl.when(has_row[vert])
                def _(vert=vert, top=top):
                    for ref in row_refs:
                        for i in range(DEEP):
                            for side in range(2):
                                end = ref[top + i, edge_at[1 - side]:edge_at[1 - side] + SUB, :]
                                ref[top + i, halo_at[side]:halo_at[side] + SUB, :] = neighbour_run(end, side)

                for side in range(2):
                    @pl.when(both(has_side[side], has_row[vert]))
                    def _(side=side, vert=vert, top=top):
                        corner_copy(1 - side, 1 - vert).wait_recv()
                        for w, ref in enumerate(row_refs):
                            packed = corner_in[side, vert, w * SUB:(w + 1) * SUB, :]
                            pairs = [((rows - DEEP if vert == 0 else 0) + i, top + i) for i in range(DEEP)]
                            unpack(ref, side, packed, pairs)

            prepare(1 - DEEP, 1)
            prepare(rows - 1, rows + DEEP - 1)
        else:
            for side in range(2):
                top = DEEP - d if side == 0 else DEEP + rows

                @pl.when(has_row[side])
                def _(which=which, side=side, top=top, cur=cur, d=d):
                    row_copy(which, 1 - side).wait_recv()
                    move_rows(row_in.at[which, side], 0, cur, top, d)

                @pl.when(jnp.logical_not(has_row[side]))
                def _(top=top, cur=cur, d=d):
                    def clear(j, c):
                        for i in range(d):
                            cur[top + i, pl.ds(j * SUB, SUB), :] = zero_plane
                        return c

                    lax.fori_loop(0, length // SUB, clear, 0)

        for j in range(1, d + 1):
            final = done + j == STEPS
            advance(
                done + j - 1,
                (0 if final else j - d, j),
                (rows - j, rows if final else rows - j + d),
            )
        done += d

    for g in range(groups):
        if not (g * SUB >= d and (g + 1) * SUB <= rows - d):
            give_back(g)
    for side in range(2):
        @pl.when(has_side[side])
        def _(side=side):
            col_copy(side).wait_send()

        for vert in range(2):
            @pl.when(both(has_side[side], has_row[vert]))
            def _(side=side, vert=vert):
                corner_copy(side, vert).wait_send()

        @pl.when(has_row[side])
        def _(side=side):
            for which in range(1, len(ROUNDS)):
                row_copy(which, side).wait_send()
    for g in range(groups):
        store(g).wait()


def shards(n_seg, n_tile, warmth, conductivity, sources):
    rows, columns = warmth.shape
    blocks = columns // LANES
    groups = rows // SUB

    def planes(a):
        return a.reshape(groups, SUB, blocks, LANES).transpose(0, 2, 1, 3).reshape(-1, LANES)

    flat = rows * blocks
    f32 = jnp.float32
    length = LANES + 2 * SUB + 2 * PAD
    plane = (rows + 2 * DEEP, length, LANES)
    assert blocks == LANES
    vmem = pltpu.VMEM
    sem = pltpu.SemaphoreType.DMA
    n = len(ROUNDS)
    out = pl.pallas_call(
        functools.partial(kernel, (rows, blocks, n_seg, n_tile)),
        out_shape=jax.ShapeDtypeStruct((flat, LANES), f32),
        in_specs=[pl.BlockSpec(memory_space=pl.ANY)] * 3,
        out_specs=pl.BlockSpec(memory_space=pl.ANY),
        scratch_shapes=[
            vmem((flat, LANES), f32), vmem((flat, LANES), f32), vmem((flat, LANES), sources.dtype), vmem((flat, LANES), f32),
        ] + [vmem(plane, f32)] * 5 + [
            vmem((rows + 2 * DEEP, (LANES // SUB + 2) * TERMS * SUB, LANES), f32),
            vmem((2, 3 * SUB, LANES), f32), vmem((2, 3 * SUB, LANES), f32),
            vmem((2, 2, 3 * SUB, LANES), f32),
            vmem((n, 2, DEEP, length, LANES), f32), vmem((n, 2, DEEP, length, LANES), f32),
            sem((3, groups)), sem((groups,)), sem((2, 2)), sem((2, 2, 2)), sem((2, 3, 2)), sem((2, n, 2)),
        ],
        compiler_params=pltpu.CompilerParams(
            collective_id=0, has_side_effects=True, vmem_limit_bytes=60 * 1024 * 1024
        ),
    )(planes(warmth), planes(conductivity), planes(sources))
    return out.reshape(groups, blocks, SUB, LANES).transpose(0, 2, 1, 3).reshape(rows, columns)


def solution(mesh):
    spec = P("tile", "seg")
    return jax.shard_map(
        functools.partial(shards, mesh.shape["seg"], mesh.shape["tile"]),
        mesh=mesh,
        in_specs=(spec, spec, spec),
        out_specs=spec,
        check_vma=False,
    )
```

```python
import functools

import jax
import jax.numpy as jnp
from jax import lax
from jax.experimental import pallas as pl
from jax.experimental.pallas import tpu as pltpu
from jax.sharding import PartitionSpec as P

STEPS = 8
ROUNDS = (4, 4)
DEEP = max(ROUNDS)
STEP_SIZE = 0.24
LANES = 128
SUB = 8
MESH = pl.DeviceIdType.MESH

PAD = 8
TERMS = 4
VMEM_KERNEL = 44 * 1024 * 1024
VMEM_LAST = 8 * 1024 * 1024
TERM_ROWS = 5 * SUB


def kernel(
    sizes, u_hbm, k_hbm, s_hbm, out_hbm,
    u_nat, k_nat, s_nat,
    u_0, u_a, u_b, k_row, s_row, coef,
    col_out, col_in, corner_in, row_out, row_in,
    load_sem, store_sem, col_sems, corner_sems, first_sems, row_sems,
):
    rows, blocks, n_seg, n_tile = sizes
    groups = rows // SUB
    tiles = blocks // SUB
    seg, tile = lax.axis_index("seg"), lax.axis_index("tile")
    lane = lax.broadcasted_iota(jnp.int32, (SUB, LANES), 1)
    sublane = lax.broadcasted_iota(jnp.int32, (SUB, LANES), 0)
    first_lane, last_lane = lane == 0, lane == LANES - 1
    has_side = (seg > 0, seg < n_seg - 1)
    has_row = (tile > 0, tile < n_tile - 1)
    side_step = (-1, 1)
    own_at = PAD + SUB
    halo_at = (PAD, own_at + LANES)
    edge_at = (own_at, own_at + LANES - SUB)
    edge_lane = (first_lane, last_lane)
    edge_id = (0, LANES - 1)
    parts = LANES // SUB
    length = LANES + 2 * SUB + 2 * PAD
    zero = jnp.float32(0.0)

    def both(a, b):
        return jnp.logical_and(a, b)

    barrier = pltpu.get_barrier_semaphore()
    count = jnp.int32(0)
    for ds in (-1, 0, 1):
        for dt in (-1, 0, 1):
            if ds == 0 and dt == 0:
                continue
            there = jnp.bool_(True)
            if ds:
                there = has_side[(ds + 1) // 2]
            if dt:
                there = both(there, has_row[(dt + 1) // 2])
            count = count + there.astype(jnp.int32)

            @pl.when(there)
            def _(ds=ds, dt=dt):
                pl.semaphore_signal(barrier, inc=1, device_id=(seg + ds, tile + dt), device_id_type=MESH)

    span = blocks * SUB
    sources = ((u_hbm, u_nat), (k_hbm, k_nat), (s_hbm, s_nat))
    order = [0, groups - 1] + list(range(1, groups - 1))

    def load(which, g):
        src, dst = sources[which]
        part = pl.ds(g * span, span)
        return pltpu.make_async_copy(src.at[part], dst.at[part], load_sem.at[which, g])

    for g in order:
        for which in range(3):
            load(which, g).start()

    zero_plane = jnp.zeros((SUB, LANES), jnp.float32)
    for side in range(2):
        top = 0 if side == 0 else DEEP + rows

        @pl.when(jnp.logical_not(has_row[side]))
        def _(top=top):
            def clear(j, c):
                at = pl.ds(j * SUB, SUB)
                for d in range(DEEP):
                    for ref in (u_0, k_row, s_row):
                        ref[top + d, at, :] = zero_plane
                return c

            lax.fori_loop(0, length // SUB, clear, 0)

    row_refs = (u_0, k_row, s_row)
    own = pl.ds(own_at, LANES)

    def neighbour_run(end, side):
        return jnp.where(edge_lane[side], zero, pltpu.roll(end, (1, LANES - 1)[side], 1))

    def relayout(g):
        for which in range(3):
            load(which, g).wait()

        def body(r, c):
            at = pl.ds(g * span + r, LANES, stride=SUB)
            row = DEEP + g * SUB + r
            for which, ref in enumerate(row_refs):
                plane = (u_nat, k_nat, s_nat)[which][at, :]
                if which == 2:
                    plane = jnp.where(plane != 0, jnp.float32(1.0), zero)
                plane = plane.T
                ref[row, own, :] = plane
                ref[row, halo_at[0]:halo_at[0] + SUB, :] = neighbour_run(plane[-SUB:], 0)
                ref[row, halo_at[1]:halo_at[1] + SUB, :] = neighbour_run(plane[:SUB], 1)
            return c

        lax.fori_loop(0, SUB, body, 0, unroll=4)


    def first_copy(which, side):
        ref, deep = ((u_0, ROUNDS[0]), (k_row, DEEP), (s_row, DEEP))[which]
        if side == 0:
            src, dst = pl.ds(DEEP, deep), pl.ds(DEEP + rows, deep)
        else:
            src, dst = pl.ds(DEEP + rows - deep, deep), pl.ds(DEEP - deep, deep)
        return pltpu.make_async_remote_copy(
            src_ref=ref.at[src, own], dst_ref=ref.at[dst, own],
            send_sem=first_sems.at[0, which, side], recv_sem=first_sems.at[1, which, 1 - side],
            device_id=(seg, tile + side_step[side]), device_id_type=MESH,
        )

    def first_arrival(which, side):
        ref, deep = ((u_0, ROUNDS[0]), (k_row, DEEP), (s_row, DEEP))[which]
        dst = pl.ds(DEEP - deep, deep) if side == 0 else pl.ds(DEEP + rows, deep)
        return pltpu.make_async_remote_copy(
            src_ref=ref.at[dst, own], dst_ref=ref.at[dst, own],
            send_sem=first_sems.at[0, which, side], recv_sem=first_sems.at[1, which, side],
            device_id=(seg, tile + side_step[side]), device_id_type=MESH,
        )

    relayout(0)
    relayout(groups - 1)
    pl.semaphore_wait(barrier, count)
    for side in range(2):
        @pl.when(has_row[side])
        def _(side=side):
            for which in range(3):
                first_copy(which, side).start()

    def col_copy(side):
        return pltpu.make_async_remote_copy(
            src_ref=col_out.at[side], dst_ref=col_in.at[1 - side],
            send_sem=col_sems.at[0, side], recv_sem=col_sems.at[1, 1 - side],
            device_id=(seg + side_step[side], tile), device_id_type=MESH,
        )

    def corner_copy(side, vert):
        return pltpu.make_async_remote_copy(
            src_ref=col_out.at[side],
            dst_ref=corner_in.at[1 - side, 1 - vert],
            send_sem=corner_sems.at[0, side, vert], recv_sem=corner_sems.at[1, 1 - side, 1 - vert],
            device_id=(seg + side_step[side], tile + side_step[vert]), device_id_type=MESH,
        )

    for g in range(1, groups - 1):
        relayout(g)
    for side in range(2):
        for which, ref in enumerate(row_refs):
            packed = jnp.zeros((SUB, LANES), jnp.float32)
            for r in range(rows):
                end = ref[DEEP + r, edge_at[side]:edge_at[side] + SUB, :]
                packed = jnp.where(lane == r, pltpu.roll(end, (r - edge_id[side]) % LANES, 1), packed)
            col_out[side, which * SUB:(which + 1) * SUB, :] = packed

        @pl.when(has_side[side])
        def _(side=side):
            col_copy(side).start()

        for vert in range(2):
            @pl.when(both(has_side[side], has_row[vert]))
            def _(side=side, vert=vert):
                corner_copy(side, vert).start()

    def unpack(ref, side, packed, pairs):
        at = slice(halo_at[side], halo_at[side] + SUB)
        for r, row in pairs:
            end = pltpu.roll(packed, (edge_id[side] - r) % LANES, 1)
            ref[row, at, :] = jnp.where(edge_lane[side], end, ref[row, at, :])

    half = jnp.float32(0.5 * STEP_SIZE)

    def prepare(lo, hi, first=0, end=parts + 2):
        def body(g, c):
            base = pl.multiple_of(g * SUB, SUB) + PAD
            at = pl.ds(base, SUB)
            cell = base - own_at + sublane
            outside = both(both(seg == 0, first_lane), cell < 0)
            outside = jnp.logical_or(outside, both(both(seg == n_seg - 1, last_lane), cell >= LANES))
            above, here = k_row[DEEP + lo - 1, at, :], k_row[DEEP + lo, at, :]
            for r in range(lo, hi):
                row = DEEP + r
                below = k_row[row + 1, at, :]
                live = both(jnp.logical_not(outside), s_row[row, at, :] == 0.0)
                if r < 0:
                    live = both(live, has_row[0])
                if r >= rows:
                    live = both(live, has_row[1])
                weight = jnp.where(live, half, zero)
                cw = weight * (here + k_row[row, pl.ds(base - 1, SUB), :])
                ce = weight * (here + k_row[row, pl.ds(base + 1, SUB), :])
                cn = weight * (here + above)
                cs = weight * (here + below)
                for i, term in enumerate((ce, cw, cn, cs)):
                    coef[row, pl.ds(pl.multiple_of(g * TERM_ROWS, SUB) + i * SUB, SUB), :] = term
                above, here = here, below
            return c

        lax.fori_loop(first, end, body, 0)

    def advance(step, *ranges):
        src, dst = (u_b, u_a) if step % 2 == 0 else (u_a, u_b)
        src = u_0 if step == 0 else src
        last = step == STEPS - 1

        def body(g, c):
            base = pl.multiple_of(g * SUB, SUB) + PAD
            at = pl.ds(base, SUB)
            for lo, hi in ranges:
                here = src[DEEP + lo, at, :]
                rise = here - src[DEEP + lo - 1, at, :]
                for r in range(lo, hi):
                    row = DEEP + r
                    below = src[row + 1, at, :]
                    ce, cw, cn, cs = (
                        coef[row, pl.ds(pl.multiple_of(g * TERM_ROWS, SUB) + i * SUB, SUB), :] for i in range(TERMS)
                    )
                    fall = below - here
                    new = here + (
                        (cs * fall - cn * rise)
                        + (ce * (src[row, pl.ds(base + 1, SUB), :] - here) + cw * (src[row, pl.ds(base - 1, SUB), :] - here))
                    )
                    if step == 0:
                        new = jnp.where(s_row[row, at, :] != 0.0, jnp.float32(1.0), new)
                    dst[row, at, :] = new
                    here, rise = below, fall
            return c

        lax.fori_loop(1 if last else 0, parts + (1 if last else 2), body, 0, unroll=2 if len(ranges) > 1 else 1)

    def row_copy(which, side):
        d = ROUNDS[which]
        return pltpu.make_async_remote_copy(
            src_ref=row_out.at[which, side, pl.ds(0, d)], dst_ref=row_in.at[which, 1 - side, pl.ds(0, d)],
            send_sem=row_sems.at[0, which, side], recv_sem=row_sems.at[1, which, 1 - side],
            device_id=(seg, tile + side_step[side]), device_id_type=MESH,
        )

    def move_rows(src, src_row, dst, dst_row, d):
        def body(j, c):
            at = pl.ds(j * SUB, SUB)
            for i in range(d):
                dst[dst_row + i, at, :] = src[src_row + i, at, :]
            return c

        lax.fori_loop(0, length // SUB, body, 0)

    def store(g):
        done_ref = u_b if STEPS % 2 == 0 else u_a
        return pltpu.make_async_copy(
            done_ref.at[pl.ds(DEEP + g * SUB, SUB), own], out_hbm.at[pl.ds(g * SUB, SUB)], store_sem.at[g]
        )

    done = 0
    prepare(1, rows - 1, 2, parts)
    for side in range(2):
        @pl.when(has_side[side])
        def _(side=side):
            col_copy(1 - side).wait_recv()
            for which, ref in enumerate(row_refs):
                unpack(ref, side, col_in[side, which * SUB:(which + 1) * SUB, :], [(r, DEEP + r) for r in range(rows)])
    prepare(1, rows - 1, 0, 2)
    prepare(1, rows - 1, parts, parts + 2)
    for which, d in enumerate(ROUNDS):
        if which:
            cur = u_a if done % 2 == 1 else u_b
            for side in range(2):
                move_rows(cur, DEEP if side == 0 else DEEP + rows - d, row_out.at[which, side], 0, d)

                @pl.when(has_row[side])
                def _(which=which, side=side):
                    row_copy(which, side).start()

        for j in range(1, d + 1):
            advance(done + j - 1, (j, rows - j))
        if which == len(ROUNDS) - 1:
            for g in range(1, groups - 1):
                if g * SUB >= d and (g + 1) * SUB <= rows - d:
                    store(g).start()

        if which == 0:
            for side in range(2):
                @pl.when(has_row[side])
                def _(side=side):
                    for w in range(3):
                        first_arrival(w, side).wait_recv()
                        first_copy(w, side).wait_send()

            for vert in range(2):
                top = 0 if vert == 0 else DEEP + rows

                @pl.when(has_row[vert])
                def _(vert=vert, top=top):
                    for ref in row_refs:
                        for i in range(DEEP):
                            for side in range(2):
                                end = ref[top + i, edge_at[1 - side]:edge_at[1 - side] + SUB, :]
                                ref[top + i, halo_at[side]:halo_at[side] + SUB, :] = neighbour_run(end, side)

                for side in range(2):
                    @pl.when(both(has_side[side], has_row[vert]))
                    def _(side=side, vert=vert, top=top):
                        corner_copy(1 - side, 1 - vert).wait_recv()
                        for w, ref in enumerate(row_refs):
                            packed = corner_in[side, vert, w * SUB:(w + 1) * SUB, :]
                            pairs = [((rows - DEEP if vert == 0 else 0) + i, top + i) for i in range(DEEP)]
                            unpack(ref, side, packed, pairs)

            prepare(1 - DEEP, 1)
            prepare(rows - 1, rows + DEEP - 1)
        else:
            for side in range(2):
                top = DEEP - d if side == 0 else DEEP + rows

                @pl.when(has_row[side])
                def _(which=which, side=side, top=top, cur=cur, d=d):
                    row_copy(which, 1 - side).wait_recv()
                    move_rows(row_in.at[which, side], 0, cur, top, d)

                @pl.when(jnp.logical_not(has_row[side]))
                def _(top=top, cur=cur, d=d):
                    def clear(j, c):
                        for i in range(d):
                            cur[top + i, pl.ds(j * SUB, SUB), :] = zero_plane
                        return c

                    lax.fori_loop(0, length // SUB, clear, 0)

        for j in range(1, d + 1):
            final = done + j == STEPS
            advance(
                done + j - 1,
                (0 if final else j - d, j),
                (rows - j, rows if final else rows - j + d),
            )
        done += d

    for g in range(groups):
        if not (g * SUB >= d and (g + 1) * SUB <= rows - d):
            store(g).start()
    for side in range(2):
        @pl.when(has_side[side])
        def _(side=side):
            col_copy(side).wait_send()

        for vert in range(2):
            @pl.when(both(has_side[side], has_row[vert]))
            def _(side=side, vert=vert):
                corner_copy(side, vert).wait_send()

        @pl.when(has_row[side])
        def _(side=side):
            for which in range(1, len(ROUNDS)):
                row_copy(which, side).wait_send()
    for g in range(groups):
        store(g).wait()


def give_back(planes, out):
    for r in range(SUB):
        out[pl.ds(r, LANES, stride=SUB), :] = planes[r].T


def shards(n_seg, n_tile, warmth, conductivity, sources):
    rows, columns = warmth.shape
    blocks = columns // LANES
    groups = rows // SUB

    def planes(a):
        return a.reshape(groups, SUB, blocks, LANES).transpose(0, 2, 1, 3).reshape(-1, LANES)

    flat = rows * blocks
    f32 = jnp.float32
    length = LANES + 2 * SUB + 2 * PAD
    plane = (rows + 2 * DEEP, length, LANES)
    assert blocks == LANES
    vmem = pltpu.VMEM
    sem = pltpu.SemaphoreType.DMA
    n = len(ROUNDS)
    out = pl.pallas_call(
        functools.partial(kernel, (rows, blocks, n_seg, n_tile)),
        out_shape=jax.ShapeDtypeStruct((rows, LANES, LANES), f32),
        in_specs=[pl.BlockSpec(memory_space=pl.ANY)] * 3,
        out_specs=pl.BlockSpec(memory_space=pl.ANY),
        scratch_shapes=[
            vmem((flat, LANES), f32), vmem((flat, LANES), f32), vmem((flat, LANES), sources.dtype),
        ] + [vmem(plane, f32)] * 5 + [
            vmem((rows + 2 * DEEP, (LANES // SUB + 2) * TERM_ROWS, LANES), f32),
            vmem((2, 3 * SUB, LANES), f32), vmem((2, 3 * SUB, LANES), f32),
            vmem((2, 2, 3 * SUB, LANES), f32),
            vmem((n, 2, DEEP, length, LANES), f32), vmem((n, 2, DEEP, length, LANES), f32),
            sem((3, groups)), sem((groups,)), sem((2, 2)), sem((2, 2, 2)), sem((2, 3, 2)), sem((2, n, 2)),
        ],
        compiler_params=pltpu.CompilerParams(
            collective_id=0, has_side_effects=True, vmem_limit_bytes=VMEM_KERNEL
        ),
    )(planes(warmth), planes(conductivity), planes(sources))
    out = pl.pallas_call(
        give_back,
        grid=(groups,),
        out_shape=jax.ShapeDtypeStruct((flat, LANES), f32),
        in_specs=[pl.BlockSpec((SUB, LANES, LANES), lambda g: (g, 0, 0))],
        out_specs=pl.BlockSpec((blocks * SUB, LANES), lambda g: (g, 0)),
        compiler_params=pltpu.CompilerParams(vmem_limit_bytes=VMEM_LAST),
    )(out)
    return out.reshape(groups, blocks, SUB, LANES).transpose(0, 2, 1, 3).reshape(rows, columns)


def solution(mesh):
    spec = P("tile", "seg")
    return jax.shard_map(
        functools.partial(shards, mesh.shape["seg"], mesh.shape["tile"]),
        mesh=mesh,
        in_specs=(spec, spec, spec),
        out_specs=spec,
        check_vma=False,
    )
```

```python
import functools

import jax
import jax.numpy as jnp
from jax import lax
from jax.experimental import pallas as pl
from jax.experimental.pallas import tpu as pltpu
from jax.sharding import PartitionSpec as P

STEPS = 8
ROUNDS = (4, 4)
DEEP = max(ROUNDS)
STEP_SIZE = 0.24
LANES = 128
SUB = 8
MESH = pl.DeviceIdType.MESH

PAD = 16
TERMS = 4
VMEM_KERNEL = 50 * 1024 * 1024
VMEM_LAST = 8 * 1024 * 1024
TERM_ROWS = 5 * SUB


def kernel(
    sizes, u_hbm, k_hbm, s_hbm, out_hbm,
    u_nat, k_nat, s_nat,
    u_0, u_a, u_b, k_row, s_row, coef,
    col_out, col_in, corner_in, row_out, row_in,
    load_sem, store_sem, col_sems, corner_sems, first_sems, row_sems,
):
    rows, blocks, n_seg, n_tile = sizes
    groups = rows // SUB
    tiles = blocks // SUB
    seg, tile = lax.axis_index("seg"), lax.axis_index("tile")
    lane = lax.broadcasted_iota(jnp.int32, (SUB, LANES), 1)
    sublane = lax.broadcasted_iota(jnp.int32, (SUB, LANES), 0)
    first_lane, last_lane = lane == 0, lane == LANES - 1
    has_side = (seg > 0, seg < n_seg - 1)
    has_row = (tile > 0, tile < n_tile - 1)
    side_step = (-1, 1)
    own_at = PAD + SUB
    halo_at = (PAD, own_at + LANES)
    edge_at = (own_at, own_at + LANES - SUB)
    edge_lane = (first_lane, last_lane)
    edge_id = (0, LANES - 1)
    parts = LANES // SUB
    length = LANES + 2 * SUB + 2 * PAD
    zero = jnp.float32(0.0)

    def both(a, b):
        return jnp.logical_and(a, b)

    barrier = pltpu.get_barrier_semaphore()
    count = jnp.int32(0)
    for ds in (-1, 0, 1):
        for dt in (-1, 0, 1):
            if ds == 0 and dt == 0:
                continue
            there = jnp.bool_(True)
            if ds:
                there = has_side[(ds + 1) // 2]
            if dt:
                there = both(there, has_row[(dt + 1) // 2])
            count = count + there.astype(jnp.int32)

            @pl.when(there)
            def _(ds=ds, dt=dt):
                pl.semaphore_signal(barrier, inc=1, device_id=(seg + ds, tile + dt), device_id_type=MESH)

    span = blocks * SUB
    sources = ((u_hbm, u_nat), (k_hbm, k_nat), (s_hbm, s_nat))
    order = [0, groups - 1] + list(range(1, groups - 1))

    def load(which, g):
        src, dst = sources[which]
        part = pl.ds(g * span, span)
        return pltpu.make_async_copy(src.at[part], dst.at[part], load_sem.at[which, g])

    for g in order:
        for which in range(3):
            load(which, g).start()

    zero_plane = jnp.zeros((SUB, LANES), jnp.float32)
    for side in range(2):
        top = 0 if side == 0 else DEEP + rows

        @pl.when(jnp.logical_not(has_row[side]))
        def _(top=top):
            def clear(j, c):
                at = pl.ds(j * SUB, SUB)
                for d in range(DEEP):
                    for ref in (u_0, k_row, s_row):
                        ref[top + d, at, :] = zero_plane
                return c

            lax.fori_loop(0, length // SUB, clear, 0)

    row_refs = (u_0, k_row, s_row)
    own = pl.ds(own_at, LANES)

    def neighbour_run(end, side):
        return jnp.where(edge_lane[side], zero, pltpu.roll(end, (1, LANES - 1)[side], 1))

    def relayout(g):
        for which in range(3):
            load(which, g).wait()

        def body(r, c):
            at = pl.ds(g * span + r, LANES, stride=SUB)
            row = DEEP + g * SUB + r
            for which, ref in enumerate(row_refs):
                plane = (u_nat, k_nat, s_nat)[which][at, :]
                if which == 2:
                    plane = jnp.where(plane != 0, jnp.float32(1.0), zero)
                plane = plane.T
                ref[row, own, :] = plane
                ref[row, halo_at[0]:halo_at[0] + SUB, :] = neighbour_run(plane[-SUB:], 0)
                ref[row, halo_at[1]:halo_at[1] + SUB, :] = neighbour_run(plane[:SUB], 1)
            return c

        lax.fori_loop(0, SUB, body, 0, unroll=4)


    def first_copy(which, side):
        ref, deep = ((u_0, ROUNDS[0]), (k_row, DEEP), (s_row, DEEP))[which]
        if side == 0:
            src, dst = pl.ds(DEEP, deep), pl.ds(DEEP + rows, deep)
        else:
            src, dst = pl.ds(DEEP + rows - deep, deep), pl.ds(DEEP - deep, deep)
        return pltpu.make_async_remote_copy(
            src_ref=ref.at[src, own], dst_ref=ref.at[dst, own],
            send_sem=first_sems.at[0, which, side], recv_sem=first_sems.at[1, which, 1 - side],
            device_id=(seg, tile + side_step[side]), device_id_type=MESH,
        )

    def first_arrival(which, side):
        ref, deep = ((u_0, ROUNDS[0]), (k_row, DEEP), (s_row, DEEP))[which]
        dst = pl.ds(DEEP - deep, deep) if side == 0 else pl.ds(DEEP + rows, deep)
        return pltpu.make_async_remote_copy(
            src_ref=ref.at[dst, own], dst_ref=ref.at[dst, own],
            send_sem=first_sems.at[0, which, side], recv_sem=first_sems.at[1, which, side],
            device_id=(seg, tile + side_step[side]), device_id_type=MESH,
        )

    relayout(0)
    relayout(groups - 1)
    pl.semaphore_wait(barrier, count)
    for side in range(2):
        @pl.when(has_row[side])
        def _(side=side):
            for which in range(3):
                first_copy(which, side).start()

    def col_copy(side):
        return pltpu.make_async_remote_copy(
            src_ref=col_out.at[side], dst_ref=col_in.at[1 - side],
            send_sem=col_sems.at[0, side], recv_sem=col_sems.at[1, 1 - side],
            device_id=(seg + side_step[side], tile), device_id_type=MESH,
        )

    def corner_copy(side, vert):
        return pltpu.make_async_remote_copy(
            src_ref=col_out.at[side],
            dst_ref=corner_in.at[1 - side, 1 - vert],
            send_sem=corner_sems.at[0, side, vert], recv_sem=corner_sems.at[1, 1 - side, 1 - vert],
            device_id=(seg + side_step[side], tile + side_step[vert]), device_id_type=MESH,
        )

    for g in range(1, groups - 1):
        relayout(g)
    for side in range(2):
        for which, ref in enumerate(row_refs):
            packed = jnp.zeros((SUB, LANES), jnp.float32)
            for r in range(rows):
                end = ref[DEEP + r, edge_at[side]:edge_at[side] + SUB, :]
                packed = jnp.where(lane == r, pltpu.roll(end, (r - edge_id[side]) % LANES, 1), packed)
            col_out[side, which * SUB:(which + 1) * SUB, :] = packed

        @pl.when(has_side[side])
        def _(side=side):
            col_copy(side).start()

        for vert in range(2):
            @pl.when(both(has_side[side], has_row[vert]))
            def _(side=side, vert=vert):
                corner_copy(side, vert).start()

    def unpack(ref, side, packed, pairs):
        at = slice(halo_at[side], halo_at[side] + SUB)
        for r, row in pairs:
            end = pltpu.roll(packed, (edge_id[side] - r) % LANES, 1)
            ref[row, at, :] = jnp.where(edge_lane[side], end, ref[row, at, :])

    half = jnp.float32(0.5 * STEP_SIZE)

    def prepare(lo, hi, first=0, end=parts + 2):
        def body(g, c):
            base = pl.multiple_of(g * SUB, SUB) + PAD
            at = pl.ds(base, SUB)
            cell = base - own_at + sublane
            outside = both(both(seg == 0, first_lane), cell < 0)
            outside = jnp.logical_or(outside, both(both(seg == n_seg - 1, last_lane), cell >= LANES))
            above, here = k_row[DEEP + lo - 1, at, :], k_row[DEEP + lo, at, :]
            for r in range(lo, hi):
                row = DEEP + r
                below = k_row[row + 1, at, :]
                live = both(jnp.logical_not(outside), s_row[row, at, :] == 0.0)
                if r < 0:
                    live = both(live, has_row[0])
                if r >= rows:
                    live = both(live, has_row[1])
                weight = jnp.where(live, half, zero)
                cw = weight * (here + k_row[row, pl.ds(base - 1, SUB), :])
                ce = weight * (here + k_row[row, pl.ds(base + 1, SUB), :])
                cn = weight * (here + above)
                cs = weight * (here + below)
                for i, term in enumerate((ce, cw, cn, cs)):
                    coef[row, pl.ds(pl.multiple_of(g * TERM_ROWS, SUB) + i * SUB, SUB), :] = term
                above, here = here, below
            return c

        lax.fori_loop(first, end, body, 0)

    def advance(step, *ranges):
        src, dst = (u_b, u_a) if step % 2 == 0 else (u_a, u_b)
        src = u_0 if step == 0 else src
        last = step == STEPS - 1

        def body(g, c):
            base = pl.multiple_of(g * SUB, SUB) + PAD
            at = pl.ds(base, SUB)
            for lo, hi in ranges:
                here = src[DEEP + lo, at, :]
                rise = here - src[DEEP + lo - 1, at, :]
                for r in range(lo, hi):
                    row = DEEP + r
                    below = src[row + 1, at, :]
                    ce, cw, cn, cs = (
                        coef[row, pl.ds(pl.multiple_of(g * TERM_ROWS, SUB) + i * SUB, SUB), :] for i in range(TERMS)
                    )
                    fall = below - here
                    new = here + (
                        (cs * fall - cn * rise)
                        + (ce * (src[row, pl.ds(base + 1, SUB), :] - here) + cw * (src[row, pl.ds(base - 1, SUB), :] - here))
                    )
                    if step == 0:
                        new = jnp.where(s_row[row, at, :] != 0.0, jnp.float32(1.0), new)
                    dst[row, at, :] = new
                    here, rise = below, fall
            return c

        lax.fori_loop(1 if last else 0, parts + (1 if last else 2), body, 0, unroll=2 if len(ranges) > 1 else 1)

    def row_copy(which, side):
        d = ROUNDS[which]
        return pltpu.make_async_remote_copy(
            src_ref=row_out.at[which, side, pl.ds(0, d)], dst_ref=row_in.at[which, 1 - side, pl.ds(0, d)],
            send_sem=row_sems.at[0, which, side], recv_sem=row_sems.at[1, which, 1 - side],
            device_id=(seg, tile + side_step[side]), device_id_type=MESH,
        )

    def move_rows(src, src_row, src_at, dst, dst_row, dst_at, d):
        def body(j, c):
            for i in range(d):
                dst[dst_row + i, pl.ds(dst_at + j * SUB, SUB), :] = src[src_row + i, pl.ds(src_at + j * SUB, SUB), :]
            return c

        lax.fori_loop(0, parts + 2, body, 0)

    def store(g):
        done_ref = u_b if STEPS % 2 == 0 else u_a
        return pltpu.make_async_copy(
            done_ref.at[pl.ds(DEEP + g * SUB, SUB), own], out_hbm.at[pl.ds(g * SUB, SUB)], store_sem.at[g]
        )

    done = 0
    prepare(1, rows - 1, 2, parts)
    for side in range(2):
        @pl.when(has_side[side])
        def _(side=side):
            col_copy(1 - side).wait_recv()
            for which, ref in enumerate(row_refs):
                unpack(ref, side, col_in[side, which * SUB:(which + 1) * SUB, :], [(r, DEEP + r) for r in range(rows)])
    prepare(1, rows - 1, 0, 2)
    prepare(1, rows - 1, parts, parts + 2)
    for which, d in enumerate(ROUNDS):
        if which:
            cur = u_a if done % 2 == 1 else u_b
            for side in range(2):
                move_rows(cur, DEEP if side == 0 else DEEP + rows - d, PAD, row_out.at[which, side], 0, 0, d)

                @pl.when(has_row[side])
                def _(which=which, side=side):
                    row_copy(which, side).start()

        for j in range(1, d + 1):
            advance(done + j - 1, (j, rows - j))
        if which == len(ROUNDS) - 1:
            for g in range(1, groups - 1):
                if g * SUB >= d and (g + 1) * SUB <= rows - d:
                    store(g).start()

        if which == 0:
            for side in range(2):
                @pl.when(has_row[side])
                def _(side=side):
                    for w in range(3):
                        first_arrival(w, side).wait_recv()
                        first_copy(w, side).wait_send()

            for vert in range(2):
                top = 0 if vert == 0 else DEEP + rows

                @pl.when(has_row[vert])
                def _(vert=vert, top=top):
                    for ref in row_refs:
                        for i in range(DEEP):
                            for side in range(2):
                                end = ref[top + i, edge_at[1 - side]:edge_at[1 - side] + SUB, :]
                                ref[top + i, halo_at[side]:halo_at[side] + SUB, :] = neighbour_run(end, side)

                for side in range(2):
                    @pl.when(both(has_side[side], has_row[vert]))
                    def _(side=side, vert=vert, top=top):
                        corner_copy(1 - side, 1 - vert).wait_recv()
                        for w, ref in enumerate(row_refs):
                            packed = corner_in[side, vert, w * SUB:(w + 1) * SUB, :]
                            pairs = [((rows - DEEP if vert == 0 else 0) + i, top + i) for i in range(DEEP)]
                            unpack(ref, side, packed, pairs)

            prepare(1 - DEEP, 1)
            prepare(rows - 1, rows + DEEP - 1)
        else:
            for side in range(2):
                top = DEEP - d if side == 0 else DEEP + rows

                @pl.when(has_row[side])
                def _(which=which, side=side, top=top, cur=cur, d=d):
                    row_copy(which, 1 - side).wait_recv()
                    move_rows(row_in.at[which, side], 0, 0, cur, top, PAD, d)

                @pl.when(jnp.logical_not(has_row[side]))
                def _(top=top, cur=cur, d=d):
                    def clear(j, c):
                        for i in range(d):
                            cur[top + i, pl.ds(j * SUB, SUB), :] = zero_plane
                        return c

                    lax.fori_loop(0, length // SUB, clear, 0)

        for j in range(1, d + 1):
            final = done + j == STEPS
            advance(
                done + j - 1,
                (0 if final else j - d, j),
                (rows - j, rows if final else rows - j + d),
            )
        done += d

    for g in range(groups):
        if not (g * SUB >= d and (g + 1) * SUB <= rows - d):
            store(g).start()
    for side in range(2):
        @pl.when(has_side[side])
        def _(side=side):
            col_copy(side).wait_send()

        for vert in range(2):
            @pl.when(both(has_side[side], has_row[vert]))
            def _(side=side, vert=vert):
                corner_copy(side, vert).wait_send()

        @pl.when(has_row[side])
        def _(side=side):
            for which in range(1, len(ROUNDS)):
                row_copy(which, side).wait_send()
    for g in range(groups):
        store(g).wait()


def give_back(planes, out):
    for r in range(SUB):
        out[pl.ds(r, LANES, stride=SUB), :] = planes[r].T


def shards(n_seg, n_tile, warmth, conductivity, sources):
    rows, columns = warmth.shape
    blocks = columns // LANES
    groups = rows // SUB

    def planes(a):
        return a.reshape(groups, SUB, blocks, LANES).transpose(0, 2, 1, 3).reshape(-1, LANES)

    flat = rows * blocks
    f32 = jnp.float32
    length = LANES + 2 * SUB + 2 * PAD
    plane = (rows + 2 * DEEP, length, LANES)
    assert blocks == LANES
    vmem = pltpu.VMEM
    sem = pltpu.SemaphoreType.DMA
    n = len(ROUNDS)
    out = pl.pallas_call(
        functools.partial(kernel, (rows, blocks, n_seg, n_tile)),
        out_shape=jax.ShapeDtypeStruct((rows, LANES, LANES), f32),
        in_specs=[pl.BlockSpec(memory_space=pltpu.HBM)] * 3,
        out_specs=pl.BlockSpec(memory_space=pl.ANY),
        scratch_shapes=[
            vmem((flat, LANES), f32), vmem((flat, LANES), f32), vmem((flat, LANES), sources.dtype),
        ] + [vmem(plane, f32)] * 5 + [
            vmem((rows + 2 * DEEP, (LANES // SUB + 2) * TERM_ROWS, LANES), f32),
            vmem((2, 3 * SUB, LANES), f32), vmem((2, 3 * SUB, LANES), f32),
            vmem((2, 2, 3 * SUB, LANES), f32),
            vmem((n, 2, DEEP, LANES + 2 * SUB, LANES), f32), vmem((n, 2, DEEP, LANES + 2 * SUB, LANES), f32),
            sem((3, groups)), sem((groups,)), sem((2, 2)), sem((2, 2, 2)), sem((2, 3, 2)), sem((2, n, 2)),
        ],
        compiler_params=pltpu.CompilerParams(
            collective_id=0, has_side_effects=True, vmem_limit_bytes=VMEM_KERNEL
        ),
    )(planes(warmth), planes(conductivity), planes(sources))
    out = pl.pallas_call(
        give_back,
        grid=(groups,),
        out_shape=jax.ShapeDtypeStruct((flat, LANES), f32),
        in_specs=[pl.BlockSpec((SUB, LANES, LANES), lambda g: (g, 0, 0))],
        out_specs=pl.BlockSpec((blocks * SUB, LANES), lambda g: (g, 0)),
        compiler_params=pltpu.CompilerParams(vmem_limit_bytes=VMEM_LAST),
    )(out)
    return out.reshape(groups, blocks, SUB, LANES).transpose(0, 2, 1, 3).reshape(rows, columns)


def solution(mesh):
    spec = P("tile", "seg")
    return jax.shard_map(
        functools.partial(shards, mesh.shape["seg"], mesh.shape["tile"]),
        mesh=mesh,
        in_specs=(spec, spec, spec),
        out_specs=spec,
        check_vma=False,
    )
```
